768 devices in a mesh: seq: 96 (over z, x, core), head: 8 (over y).
Axes of the slice: x: 4, y: 8, z: 12, core: 2. Of those that a mesh axis runs over, the one named last changes fastest.
Arguments:
- queries: bfloat16 [49152, 4096], P('seq', 'head'), may hold values from -360 to 360, as said below
- key_rows: bfloat16 [49152, 1024], P('seq', 'head'), may hold values from -6 to 6
- value_rows: bfloat16 [49152, 1024], P('seq', 'head'), may hold values from -6 to 6
- doc_lengths: int32 [96], replicated, may hold values from 1 to 1536, 49152 in all
Outputs:
- attn_out: bfloat16 [49152, 4096], P(('seq', 'head'))
The draws below stay inside these ranges and needn't reach their ends.
Inputs may be any that keep to these rules, and one draw needn't show every extreme that they name: `queries`: custom draw of bounded query entries. `doc_lengths`: the lengths sum to 49152; each is at most 1536.
All inputs are finite; a program needn't handle non-finite values.
Results may differ from the reference program's by a relative error of at most 0.0036.
Values may be sent and summed in bfloat16 or wider, within the bound.
No kernel may reach another device: no remote copies, remote signals or barrier semaphores. Data moves between devices by JAX's collectives and lax.ppermute only.
A program may use at most 32 MiB of HBM per device.

```python
import math
import jax
import jax.numpy as jnp
import numpy as np
from jax import lax

H = 32
KVH = 8
HD = 128
TOK_DEV = 512
SPAN = 4
TOKENS = 49152
MAXDOC = 1536
NDOCS = 96
N_SEQ = 96


def draw_queries(key, part):
    base = jnp.clip(jax.random.normal(key, (TOKENS, H * HD), jnp.float32), -4.5, 4.5)
    return base.astype(jnp.bfloat16)


def block_scale(own_key, shape, pieces, low, high):
    gain, own = 1.0, jax.random.fold_in(own_key, 6)
    for position, parts in pieces:
        heights = jnp.exp(jax.random.uniform(jax.random.fold_in(own, position), (parts,), jnp.float32, low / len(pieces), high / len(pieces)))
        gain = gain * jnp.repeat(heights, shape[position] // parts).reshape([-1 if axis == position else 1 for axis in range(len(shape))])
    return gain


def split_up(count, total, limit, slope):
    portions = [(1 << 20) // math.isqrt(standing ** slope) + 1 for standing in range(2, count + 1)]
    rest, counts = total - limit - (count - 1), [1] * (count - 1)
    while rest > 0:
        free = [i for i in range(count - 1) if counts[i] < limit]
        whole, left = sum([portions[i] for i in free]), rest
        for i in free:
            extra = min(limit - counts[i], max(1, left * portions[i] // whole), rest)
            counts[i] = counts[i] + extra
            rest = rest - extra
    return np.array([limit] + counts)


def ragged(key, amount, total, limit, slope):
    if amount == 2:
        one = jax.random.randint(key, (), max(1, total - limit), min(limit, total - 1) + 1)
        return jnp.stack([one, total - one])
    lengths = jnp.asarray(split_up(amount, total, limit, slope), jnp.int32)
    couples = (amount - 1) // 2
    source_of, sink = lengths[1:1 + 2 * couples:2], lengths[2:2 + 2 * couples:2]
    room = jnp.minimum(source_of - 1, limit - sink)
    passed = jax.random.randint(jax.random.fold_in(key, 1), (couples,), 0, 1 << 20) % (room + 1)
    lengths = lengths.at[1:1 + 2 * couples:2].set(source_of - passed).at[2:2 + 2 * couples:2].set(sink + passed)
    return lengths[jax.random.permutation(jax.random.fold_in(key, 2), amount)]


def noise(stream_key, shape, deviation, limit, split=(), kind=jnp.bfloat16):
    result = jax.random.normal(stream_key, shape, jnp.float32) * deviation
    if len(split) > 0:
        result = block_scale(stream_key, shape, split, -0.22, 0.18) * result
    return jnp.clip(result, min=-limit, max=limit).astype(kind)


def setup_inputs(seed: int = 0) -> dict:
    streams_of = jax.random.split(jax.random.key(seed), 5)
    return {
        "queries": draw_queries(jax.random.fold_in(streams_of[4], 71), 0),
        "key_rows": noise(streams_of[1], (TOKENS, KVH * HD), 1.0, 6.0, ((0, 96), (1, 8))),
        "value_rows": noise(streams_of[2], (TOKENS, KVH * HD), 1.0, 6.0, ((0, 96), (1, 8))),
        "doc_lengths": ragged(streams_of[3], NDOCS, TOKENS, MAXDOC, 2).astype(jnp.int32),
    }


scaling = 0.08838834764831845


def doc_index(ends, positions):
    return jnp.sum((ends[None, :] <= positions[:, None]).astype(jnp.int32), axis=1)


def reference(queries, key_rows, value_rows, doc_lengths):
    ends = jnp.cumsum(doc_lengths).astype(jnp.int32)
    group = H // KVH
    width = SPAN * TOK_DEV
    margin = (SPAN - 1) * TOK_DEV
    key_padded = jnp.concatenate([jnp.zeros((margin, KVH * HD), key_rows.dtype), key_rows], 0)
    value_padded = jnp.concatenate([jnp.zeros((margin, KVH * HD), value_rows.dtype), value_rows], 0)

    def block(index):
        start = (index * TOK_DEV).astype(jnp.int32)
        query_block = lax.dynamic_slice_in_dim(queries, start, TOK_DEV, 0).astype(jnp.float32).reshape(TOK_DEV, KVH, group, HD)
        key_block = lax.dynamic_slice_in_dim(key_padded, start, width, 0).astype(jnp.float32).reshape(width, KVH, HD)
        value_block = lax.dynamic_slice_in_dim(value_padded, start, width, 0).astype(jnp.float32).reshape(width, KVH, HD)
        query_pos = start + jnp.arange(TOK_DEV, dtype=jnp.int32)
        key_pos = start - margin + jnp.arange(width, dtype=jnp.int32)
        allowed = (key_pos[None, :] >= 0) & (doc_index(ends, key_pos)[None, :] == doc_index(ends, query_pos)[:, None]) & (key_pos[None, :] <= query_pos[:, None])
        scores = jnp.einsum("qgjd,kgd->gjqk", query_block, key_block, precision=lax.Precision.HIGHEST) * scaling
        scores = jnp.where(allowed[None, None], scores, jnp.float32(-1e30))
        largest = jnp.max(scores, axis=-1, keepdims=True)
        weights = jnp.where(allowed[None, None], jnp.exp(scores - largest), jnp.float32(0.0))
        total = jnp.sum(weights, axis=-1)
        rounded = lax.optimization_barrier(weights.astype(jnp.bfloat16)).astype(jnp.float32)
        output = jnp.einsum("gjqk,kgd->qgjd", rounded, value_block, precision=lax.Precision.HIGHEST)
        output = output / jnp.transpose(total, (2, 0, 1))[:, :, :, None]
        return output.reshape(TOK_DEV, H * HD).astype(jnp.bfloat16)

    blocks = lax.map(block, jnp.arange(N_SEQ, dtype=jnp.int32))
    return blocks.reshape(TOKENS, H * HD)
```

```python
import jax
import jax.numpy as jnp
from jax import lax
from jax.experimental import pallas as pl
from jax.experimental.pallas import tpu as pltpu
from jax.sharding import PartitionSpec as P

HD = 128
GROUP = 4
T = 512
LANES = 128
FAR = 4194304.0
SCALE = 0.08838834764831845 * 1.4426950408889634
QT = 256


def attention_kernel(where_ref, docs_ref, q_ref, k_ref, v_ref, x_ref, a_ref, s_ref, o_ref, kw, vw):
    first, odd = where_ref[0], where_ref[1]
    begins, ends = docs_ref[0:1, :], docs_ref[1:2, :]
    ones = jnp.ones((T, HD), jnp.bfloat16)

    def inside(base, rows):
        position = base + lax.broadcasted_iota(jnp.int32, (rows, LANES), 0)
        return (position >= begins) & (position < ends)

    def put(slot, keys, values):
        rows = pl.ds(pl.multiple_of(slot * T, T), T)
        kw[rows, :HD] = keys
        kw[rows, HD:] = jnp.where(inside(first + (slot - 3) * T, T), 0.0, -FAR).astype(jnp.bfloat16)
        vw[rows, :HD] = values
        vw[rows, HD:] = ones

    put(3, k_ref[...], v_ref[...])
    put(1, a_ref[:, :HD], a_ref[:, HD:])
    put(2 * odd, x_ref[:, :HD], x_ref[:, HD:])
    put(2 - 2 * odd, s_ref[:, :HD], s_ref[:, HD:])
    causal = lax.broadcasted_iota(jnp.int32, (QT, QT), 1) <= lax.broadcasted_iota(jnp.int32, (QT, QT), 0)
    for low in range(0, T, QT):
        window = slice(low, low + 3 * T + QT)
        own = jnp.where(inside(first + low, QT), 1.0, 0.0).astype(jnp.bfloat16)
        for head in range(GROUP):
            columns = slice(head * HD, (head + 1) * HD)
            query = jnp.concatenate([q_ref[low : low + QT, columns], own], 1)
            scores = lax.dot_general(
                query, kw[window, :], (((1,), (1,)), ((), ())), preferred_element_type=jnp.float32
            )
            scores = jnp.concatenate(
                [scores[:, : 3 * T], jnp.where(causal, scores[:, 3 * T :], -FAR)], 1
            )
            largest = jnp.max(scores, axis=1, keepdims=True)
            weights = jnp.exp2((scores - largest) * SCALE).astype(jnp.bfloat16)
            mixed = jnp.dot(weights, vw[window, :], preferred_element_type=jnp.float32)
            o_ref[low : low + QT, columns] = (mixed[:, :HD] / mixed[:, HD:]).astype(jnp.bfloat16)


def attention(where, docs, queries, keys, values, x, a, s):
    vmem = pl.BlockSpec(memory_space=pltpu.VMEM)
    return pl.pallas_call(
        attention_kernel,
        out_shape=jax.ShapeDtypeStruct((T, GROUP * HD), jnp.bfloat16),
        in_specs=[pl.BlockSpec(memory_space=pltpu.SMEM)] + [vmem] * 7,
        out_specs=vmem,
        scratch_shapes=[pltpu.VMEM((4 * T, 2 * HD), jnp.bfloat16)] * 2,
        compiler_params=pltpu.CompilerParams(vmem_limit_bytes=32 << 20),
        cost_estimate=pl.CostEstimate(flops=4 * 10**9, transcendentals=4 * 10**6, bytes_accessed=3 * 10**6),
        name="attention",
    )(where, docs, queries, keys, values, x, a, s)


def per_device(queries, key_rows, value_rows, doc_lengths):
    blocks = lax.axis_size("seq")
    block = lax.axis_index("seq")
    rows = jnp.concatenate([key_rows, value_rows], 1)
    a = lax.ppermute(rows, "seq", [(i, i + 2) for i in range(blocks - 2)])
    hops = [(i, i + 1 if i % 2 == 0 else i + 3) for i in range(blocks)]
    x = lax.ppermute(rows, "seq", [(i, j) for i, j in hops if j < blocks])
    s = lax.ppermute(a, "seq", [(i, i ^ 1) for i in range(blocks)])
    lengths = jnp.pad(doc_lengths, (0, LANES - doc_lengths.shape[0]))
    index = jnp.arange(LANES, dtype=jnp.int32)
    ends = jnp.sum(jnp.where(index[:, None] >= index[None, :], lengths[None, :], 0), axis=1)
    docs = jnp.stack([ends - lengths, ends])
    where = jnp.stack([block * T, block % 2]).astype(jnp.int32)
    merged = attention(where, docs, queries, key_rows, value_rows, x, a, s)
    return lax.all_to_all(merged, "head", split_axis=0, concat_axis=1, tiled=True)


def solution(mesh):
    in_specs = (P("seq", "head"), P("seq", "head"), P("seq", "head"), P())
    out_specs = P(("seq", "head"), None)
    return jax.shard_map(
        per_device, mesh=mesh, in_specs=in_specs, out_specs=out_specs, check_vma=False
    )
```

```python
import functools

import jax
import jax.numpy as jnp
from jax import lax
from jax.experimental import pallas as pl
from jax.experimental.pallas import tpu as pltpu
from jax.sharding import PartitionSpec as P


HD = 128
GROUP = 4
T = 512
LANES = 128
FAR = 4194304.0
SCALE = 0.08838834764831845 * 1.4426950408889634
QT = 256
HEADS = 4


def inside(docs_ref, base, rows):
    position = base + lax.broadcasted_iota(jnp.int32, (rows, LANES), 0)
    return (position >= docs_ref[0:1, :]) & (position < docs_ref[1:2, :])


def attend(causal, start, last, backs, where_ref, docs_ref, q_ref, *refs):
    refs = list(refs)
    first, odd = where_ref[0], where_ref[1]
    state = None if start else (refs.pop(0), refs.pop(0))
    blocks = [refs.pop(0) for _ in backs]
    if start:
        sem, q_hbm, q_ref = refs.pop(), q_ref, refs.pop(0)
        fetch = pltpu.make_async_copy(q_hbm, q_ref, sem)
        fetch.start()
    kw, vw = refs[-2:]
    outs = refs[:-2]
    for i, (even_back, odd_back) in enumerate(backs):
        rows = slice(i * T, (i + 1) * T)
        base = first - (even_back + odd * (odd_back - even_back)) * T
        kw[rows, :HD] = blocks[i][:T, :]
        kw[rows, HD:] = jnp.where(inside(docs_ref, base, T), 0.0, -FAR).astype(jnp.bfloat16)
        vw[rows, :HD] = blocks[i][T:, :]
        vw[rows, HD:] = jnp.ones((T, HD), jnp.bfloat16)
    below = None
    if causal:
        row = lax.broadcasted_iota(jnp.int32, (HEADS * QT, QT), 0) % QT
        below = lax.broadcasted_iota(jnp.int32, (HEADS * QT, QT), 1) <= row
    owns = [
        jnp.where(inside(docs_ref, first + low, QT), 1.0, 0.0).astype(jnp.bfloat16) for low in range(0, T, QT)
    ]

    def width(unit):
        return unit[0] * QT + QT if causal else len(backs) * T

    def score(unit):
        tile, head = unit
        rows = slice(tile * QT, tile * QT + QT)
        query = jnp.concatenate(
            [
                jnp.concatenate([q_ref[rows, h * HD : (h + 1) * HD], owns[tile]], 1)
                for h in range(head, head + HEADS)
            ],
            0,
        )
        scores = lax.dot_general(
            query, kw[: width(unit), :], (((1,), (1,)), ((), ())), preferred_element_type=jnp.float32
        )
        if causal:
            low = tile * QT
            tail = jnp.where(below, scores[:, low:], -FAR)
            scores = tail if low == 0 else jnp.concatenate([scores[:, :low], tail], 1)
        return scores

    def mix(unit, scores):
        tile, head = unit
        at = (tile * GROUP + head) * QT
        rows = slice(at, at + HEADS * QT)
        largest = jnp.max(scores, axis=1, keepdims=True)
        if start:
            weights = jnp.exp2((scores - largest) * SCALE).astype(jnp.bfloat16)
        else:
            before = state[0][rows, :]
            largest = jnp.maximum(before, largest)
            shrink = jnp.exp2((before - largest) * SCALE)
            weights = jnp.exp2((scores - jnp.concatenate([largest] * (width(unit) // HD), 1)) * SCALE)
            weights = weights.astype(jnp.bfloat16)
        mixed = jnp.dot(weights, vw[: width(unit), :], preferred_element_type=jnp.float32)
        top, total = mixed[:, :HD], mixed[:, HD:]
        if not start:
            top = top + state[1][rows, :HD] * shrink
            total = total + state[1][rows, HD:] * shrink
        if last:
            result = (top / total).astype(jnp.bfloat16)
            for i in range(HEADS):
                columns = slice((head + i) * HD, (head + i + 1) * HD)
                outs[0][tile * QT : tile * QT + QT, columns] = result[i * QT : (i + 1) * QT]
        else:
            outs[0][rows, :] = jnp.broadcast_to(largest, (HEADS * QT, HD))
            outs[1][rows, :HD] = top
            outs[1][rows, HD:] = total

    units = [(tile, head) for tile in range(T // QT) for head in range(0, GROUP, HEADS)]
    if start:
        fetch.wait()
    ahead = score(units[0])
    for i, unit in enumerate(units):
        scores, ahead = ahead, score(units[i + 1]) if i + 1 < len(units) else None
        mix(unit, scores)


STATE = [
    jax.ShapeDtypeStruct((GROUP * T, HD), jnp.float32),
    jax.ShapeDtypeStruct((GROUP * T, 2 * HD), jnp.float32),
]
RESULT = [jax.ShapeDtypeStruct((T, GROUP * HD), jnp.bfloat16)]


def in_hbm(x):
    return pltpu.with_memory_space_constraint(x, pltpu.HBM)


def stage(where, docs, queries, state, blocks, backs, causal=False, last=False):
    vmem = pl.BlockSpec(memory_space=pltpu.VMEM)
    start = not state
    out_shape = RESULT if last else STATE
    scratch = [pltpu.VMEM((len(blocks) * T, 2 * HD), jnp.bfloat16)] * 2
    if start:
        out_shape = [jax.ShapeDtypeStruct(queries.shape, queries.dtype)] + out_shape
        scratch.append(pltpu.SemaphoreType.DMA(()))
    args = (*state, *blocks)
    return pl.pallas_call(
        functools.partial(attend, causal, start, last, backs),
        out_shape=out_shape,
        in_specs=[pl.BlockSpec(memory_space=pltpu.SMEM), vmem, pl.BlockSpec(memory_space=pltpu.HBM) if start else vmem]
        + [vmem] * len(args),
        out_specs=[vmem] * len(out_shape),
        scratch_shapes=scratch,
        compiler_params=pltpu.CompilerParams(vmem_limit_bytes=28 << 20),
        cost_estimate=pl.CostEstimate(
            flops=10**9 * len(blocks), transcendentals=10**6 * len(blocks), bytes_accessed=10**6
        ),
    )(where, docs, in_hbm(queries) if start else queries, *args)


def pack_kernel(k_ref, v_ref, lengths_ref, rows_ref, docs_ref, lengths, sems):
    copies = [
        pltpu.make_async_copy(lengths_ref, lengths, sems.at[0]),
        pltpu.make_async_copy(k_ref, rows_ref.at[:T, :], sems.at[1]),
        pltpu.make_async_copy(v_ref, rows_ref.at[T:, :], sems.at[2]),
    ]
    for copy in copies:
        copy.start()
    copies[0].wait()
    lane = lax.broadcasted_iota(jnp.int32, (1, LANES), 1)
    begins = jnp.full((1, LANES), 1 << 30, jnp.int32)
    ends = begins
    reached = jnp.int32(0)
    for i in range(lengths.shape[0]):
        begins = jnp.where(lane == i, reached, begins)
        reached = reached + lengths[i]
        ends = jnp.where(lane == i, reached, ends)
    docs_ref[0:1, :] = begins
    docs_ref[1:2, :] = ends
    copies[1].wait()
    copies[2].wait()


def pack(keys, values, doc_lengths):
    vmem = pl.BlockSpec(memory_space=pltpu.VMEM)
    return pl.pallas_call(
        pack_kernel,
        out_shape=[pltpu.VMEM((2 * T, HD), jnp.bfloat16), pltpu.VMEM((2, LANES), jnp.int32)],
        in_specs=[pl.BlockSpec(memory_space=pltpu.HBM)] * 3,
        out_specs=[vmem, vmem],
        scratch_shapes=[pltpu.SMEM(doc_lengths.shape, jnp.int32), pltpu.SemaphoreType.DMA((3,))],
        name="pack",
    )(*(in_hbm(x) for x in (keys, values, doc_lengths)))


def per_device(queries, key_rows, value_rows, doc_lengths):
    blocks = lax.axis_size("seq")
    block = lax.axis_index("seq")
    rows, docs = pack(key_rows, value_rows, doc_lengths)
    a = lax.ppermute(rows, "seq", [(i, i + 2) for i in range(blocks - 2)])
    hops = [(i, i + 1 if i % 2 == 0 else i + 3) for i in range(blocks)]
    x = lax.ppermute(rows, "seq", [(i, j) for i, j in hops if j < blocks])
    s = lax.ppermute(a, "seq", [(i, i ^ 1) for i in range(blocks)])
    where = jnp.stack([block * T, block % 2]).astype(jnp.int32)
    near, *state = stage(where, docs, queries, (), (rows,), ((0, 0),), causal=True)
    state = stage(where, docs, near, state, (a,), ((2, 2),))
    (merged,) = stage(where, docs, near, state, (s, x), ((1, 3), (3, 1)), last=True)
    return lax.all_to_all(merged, "head", split_axis=0, concat_axis=1, tiled=True)


def solution(mesh):
    in_specs = (P("seq", "head"), P("seq", "head"), P("seq", "head"), P())
    out_specs = P(("seq", "head"), None)
    return jax.shard_map(per_device, mesh=mesh, in_specs=in_specs, out_specs=out_specs, check_vma=False)
```

```python
import functools

import jax
import jax.numpy as jnp
from jax import lax
from jax.experimental import pallas as pl
from jax.experimental.pallas import tpu as pltpu
from jax.sharding import PartitionSpec as P


HD = 128
GROUP = 4
T = 512
LANES = 128
FAR = 4194304.0
SCALE = 0.08838834764831845 * 1.4426950408889634
QT = 256
HEADS = 4


def inside(docs_ref, base, rows):
    position = base + lax.broadcasted_iota(jnp.int32, (rows, LANES), 0)
    return (position >= docs_ref[0:1, :]) & (position < docs_ref[1:2, :])


def attend(causal, start, last, backs, where_ref, docs_ref, q_ref, *refs):
    refs = list(refs)
    first, odd = where_ref[0], where_ref[1]
    state = None if start else (refs.pop(0), refs.pop(0))
    blocks = [refs.pop(0) for _ in backs]
    if start:
        sem, q_hbm, q_ref = refs.pop(), q_ref, refs.pop(0)
        fetch = pltpu.make_async_copy(q_hbm, q_ref, sem)
        fetch.start()
    kw, vw = refs[-2:]
    outs = refs[:-2]

    def put(slot, base, block):
        rows = pl.ds(pl.multiple_of(slot * T, T), T)
        kw[rows, :HD] = block[:T, :]
        kw[rows, HD:] = jnp.where(inside(docs_ref, base, T), 0.0, -FAR).astype(jnp.bfloat16)
        vw[rows, :HD] = block[T:, :]
        vw[rows, HD:] = jnp.ones((T, HD), jnp.bfloat16)

    count = 0
    if start:
        put(0, first, blocks[0])
    else:
        begins = docs_ref[0:1, :]
        reach = jnp.max(jnp.where(begins <= first, begins, 0).astype(jnp.float32))
        for block, (even_back, odd_back) in zip(blocks, backs):
            base = first - (even_back + odd * (odd_back - even_back)) * T
            needed = reach < (base + T).astype(jnp.float32)
            pl.when(needed)(functools.partial(put, count, base, block))
            count = count + needed.astype(jnp.int32)
    below = None
    if causal:
        row = lax.broadcasted_iota(jnp.int32, (HEADS * QT, QT), 0) % QT
        below = lax.broadcasted_iota(jnp.int32, (HEADS * QT, QT), 1) <= row
    owns = [
        jnp.where(inside(docs_ref, first + low, QT), 1.0, 0.0).astype(jnp.bfloat16) for low in range(0, T, QT)
    ]

    def width(unit, n):
        return unit[0] * QT + QT if causal else n * T

    def score(unit, n):
        tile, head = unit
        rows = slice(tile * QT, tile * QT + QT)
        query = jnp.concatenate(
            [
                jnp.concatenate([q_ref[rows, h * HD : (h + 1) * HD], owns[tile]], 1)
                for h in range(head, head + HEADS)
            ],
            0,
        )
        scores = lax.dot_general(
            query, kw[: width(unit, n), :], (((1,), (1,)), ((), ())), preferred_element_type=jnp.float32
        )
        if causal:
            low = tile * QT
            tail = jnp.where(below, scores[:, low:], -FAR)
            scores = tail if low == 0 else jnp.concatenate([scores[:, :low], tail], 1)
        return scores

    def mix(unit, n, scores):
        tile, head = unit
        at = (tile * GROUP + head) * QT
        rows = slice(at, at + HEADS * QT)
        largest = jnp.max(scores, axis=1, keepdims=True)
        if start:
            weights = jnp.exp2((scores - largest) * SCALE).astype(jnp.bfloat16)
        else:
            before = state[0][rows, :]
            largest = jnp.maximum(before, largest)
            shrink = jnp.exp2((before - largest) * SCALE)
            weights = jnp.exp2((scores - jnp.concatenate([largest] * (width(unit, n) // HD), 1)) * SCALE)
            weights = weights.astype(jnp.bfloat16)
        mixed = jnp.dot(weights, vw[: width(unit, n), :], preferred_element_type=jnp.float32)
        top, total = mixed[:, :HD], mixed[:, HD:]
        if not start:
            top = top + state[1][rows, :HD] * shrink
            total = total + state[1][rows, HD:] * shrink
        if last:
            store(unit, top, total)
        else:
            outs[0][rows, :] = jnp.broadcast_to(largest, (HEADS * QT, HD))
            outs[1][rows, :HD] = top
            outs[1][rows, HD:] = total

    def store(unit, top, total):
        tile, head = unit
        result = (top / total).astype(jnp.bfloat16)
        for i in range(HEADS):
            columns = slice((head + i) * HD, (head + i + 1) * HD)
            outs[0][tile * QT : tile * QT + QT, columns] = result[i * QT : (i + 1) * QT]

    units = [(tile, head) for tile in range(T // QT) for head in range(0, GROUP, HEADS)]

    def run(n):
        ahead = score(units[0], n)
        for i, unit in enumerate(units):
            scores, ahead = ahead, score(units[i + 1], n) if i + 1 < len(units) else None
            mix(unit, n, scores)

    def rest():
        if not last:
            outs[0][...] = state[0][...]
            outs[1][...] = state[1][...]
            return
        for tile, head in units:
            rows = slice((tile * GROUP + head) * QT, (tile * GROUP + head + HEADS) * QT)
            store((tile, head), state[1][rows, :HD], state[1][rows, HD:])

    if start:
        fetch.wait()
        run(1)
    else:
        for n in range(1, len(blocks) + 1):
            pl.when(count == n)(functools.partial(run, n))
        pl.when(count == 0)(rest)


STATE = [
    jax.ShapeDtypeStruct((GROUP * T, HD), jnp.float32),
    jax.ShapeDtypeStruct((GROUP * T, 2 * HD), jnp.float32),
]
RESULT = [jax.ShapeDtypeStruct((T, GROUP * HD), jnp.bfloat16)]


def in_hbm(x):
    return pltpu.with_memory_space_constraint(x, pltpu.HBM)


def stage(where, docs, queries, state, blocks, backs, causal=False, last=False):
    vmem = pl.BlockSpec(memory_space=pltpu.VMEM)
    start = not state
    out_shape = RESULT if last else STATE
    scratch = [pltpu.VMEM((len(blocks) * T, 2 * HD), jnp.bfloat16)] * 2
    if start:
        out_shape = [jax.ShapeDtypeStruct(queries.shape, queries.dtype)] + out_shape
        scratch.append(pltpu.SemaphoreType.DMA(()))
    args = (*state, *blocks)
    return pl.pallas_call(
        functools.partial(attend, causal, start, last, backs),
        out_shape=out_shape,
        in_specs=[pl.BlockSpec(memory_space=pltpu.SMEM), vmem, pl.BlockSpec(memory_space=pltpu.HBM) if start else vmem]
        + [vmem] * len(args),
        out_specs=[vmem] * len(out_shape),
        scratch_shapes=scratch,
        compiler_params=pltpu.CompilerParams(vmem_limit_bytes=28 << 20),
        cost_estimate=pl.CostEstimate(
            flops=10**9 * len(blocks), transcendentals=10**6 * len(blocks), bytes_accessed=10**6
        ),
    )(where, docs, in_hbm(queries) if start else queries, *args)


def pack_kernel(k_ref, v_ref, lengths_ref, rows_ref, docs_ref, lengths, sems):
    copies = [
        pltpu.make_async_copy(lengths_ref, lengths, sems.at[0]),
        pltpu.make_async_copy(k_ref, rows_ref.at[:T, :], sems.at[1]),
        pltpu.make_async_copy(v_ref, rows_ref.at[T:, :], sems.at[2]),
    ]
    for copy in copies:
        copy.start()
    copies[0].wait()
    lane = lax.broadcasted_iota(jnp.int32, (1, LANES), 1)
    begins = jnp.full((1, LANES), 1 << 30, jnp.int32)
    ends = begins
    reached = jnp.int32(0)
    for i in range(lengths.shape[0]):
        begins = jnp.where(lane == i, reached, begins)
        reached = reached + lengths[i]
        ends = jnp.where(lane == i, reached, ends)
    docs_ref[0:1, :] = begins
    docs_ref[1:2, :] = ends
    copies[1].wait()
    copies[2].wait()


def pack(keys, values, doc_lengths):
    vmem = pl.BlockSpec(memory_space=pltpu.VMEM)
    return pl.pallas_call(
        pack_kernel,
        out_shape=[pltpu.VMEM((2 * T, HD), jnp.bfloat16), pltpu.VMEM((2, LANES), jnp.int32)],
        in_specs=[pl.BlockSpec(memory_space=pltpu.HBM)] * 3,
        out_specs=[vmem, vmem],
        scratch_shapes=[pltpu.SMEM(doc_lengths.shape, jnp.int32), pltpu.SemaphoreType.DMA((3,))],
        name="pack",
    )(*(in_hbm(x) for x in (keys, values, doc_lengths)))


def per_device(queries, key_rows, value_rows, doc_lengths):
    blocks = lax.axis_size("seq")
    block = lax.axis_index("seq")
    rows, docs = pack(key_rows, value_rows, doc_lengths)
    a = lax.ppermute(rows, "seq", [(i, i + 2) for i in range(blocks - 2)])
    hops = [(i, i + 1 if i % 2 == 0 else i + 3) for i in range(blocks)]
    x = lax.ppermute(rows, "seq", [(i, j) for i, j in hops if j < blocks])
    s = lax.ppermute(a, "seq", [(i, i ^ 1) for i in range(blocks)])
    where = jnp.stack([block * T, block % 2]).astype(jnp.int32)
    near, *state = stage(where, docs, queries, (), (rows,), ((0, 0),), causal=True)
    state = stage(where, docs, near, state, (a,), ((2, 2),))
    (merged,) = stage(where, docs, near, state, (s, x), ((1, 3), (3, 1)), last=True)
    return lax.all_to_all(merged, "head", split_axis=0, concat_axis=1, tiled=True)


def solution(mesh):
    in_specs = (P("seq", "head"), P("seq", "head"), P("seq", "head"), P())
    out_specs = P(("seq", "head"), None)
    return jax.shard_map(per_device, mesh=mesh, in_specs=in_specs, out_specs=out_specs, check_vma=False)
```

```python
import functools

import jax
import jax.numpy as jnp
from jax import lax
from jax.experimental import pallas as pl
from jax.experimental.pallas import tpu as pltpu
from jax.sharding import PartitionSpec as P


HD = 128
GROUP = 4
T = 512
LANES = 128
FAR = 4194304.0
SCALE = 0.08838834764831845 * 1.4426950408889634
QT = 256
HEADS = 4


def inside(docs_ref, base, rows):
    position = base + lax.broadcasted_iota(jnp.int32, (rows, LANES), 0)
    return (position >= docs_ref[0:1, :]) & (position < docs_ref[1:2, :])


def attend(causal, start, last, backs, docs_ref, q_ref, *refs):
    refs = list(refs)
    place = lax.axis_index("seq")
    first, odd = place * T, place % 2
    state = None if start else (refs.pop(0), refs.pop(0))
    blocks = [refs.pop(0) for _ in backs]
    if start:
        sem, q_hbm, q_ref = refs.pop(), q_ref, refs.pop(0)
        fetch = pltpu.make_async_copy(q_hbm, q_ref, sem)
        fetch.start()
    kw, vw = refs[-2:]
    outs = refs[:-2]

    def put(slot, base, block):
        rows = pl.ds(pl.multiple_of(slot * T, T), T)
        kw[rows, :HD] = block[:T, :]
        kw[rows, HD:] = jnp.where(inside(docs_ref, base, T), 0.0, -FAR).astype(jnp.bfloat16)
        vw[rows, :HD] = block[T:, :]
        vw[rows, HD:] = jnp.ones((T, HD), jnp.bfloat16)

    count = 0
    if start:
        put(0, first, blocks[0])
    else:
        begins = docs_ref[0:1, :]
        reach = jnp.max(jnp.where(begins <= first, begins, 0).astype(jnp.float32))
        for block, (even_back, odd_back) in zip(blocks, backs):
            base = first - (even_back + odd * (odd_back - even_back)) * T
            needed = reach < (base + T).astype(jnp.float32)
            pl.when(needed)(functools.partial(put, count, base, block))
            count = count + needed.astype(jnp.int32)
    below = None
    if causal:
        row = lax.broadcasted_iota(jnp.int32, (HEADS * QT, QT), 0) % QT
        below = lax.broadcasted_iota(jnp.int32, (HEADS * QT, QT), 1) <= row
    owns = [
        jnp.where(inside(docs_ref, first + low, QT), 1.0, 0.0).astype(jnp.bfloat16) for low in range(0, T, QT)
    ]

    def width(unit, n):
        return unit[0] * QT + QT if causal else n * T

    def score(unit, n):
        tile, head = unit
        rows = slice(tile * QT, tile * QT + QT)
        query = jnp.concatenate(
            [
                jnp.concatenate([q_ref[rows, h * HD : (h + 1) * HD], owns[tile]], 1)
                for h in range(head, head + HEADS)
            ],
            0,
        )
        scores = lax.dot_general(
            query, kw[: width(unit, n), :], (((1,), (1,)), ((), ())), preferred_element_type=jnp.float32
        )
        if causal:
            low = tile * QT
            tail = jnp.where(below, scores[:, low:], -FAR)
            scores = tail if low == 0 else jnp.concatenate([scores[:, :low], tail], 1)
        return scores

    def mix(unit, n, scores):
        tile, head = unit
        at = (tile * GROUP + head) * QT
        rows = slice(at, at + HEADS * QT)
        largest = jnp.max(scores, axis=1, keepdims=True)
        if start:
            weights = jnp.exp2((scores - largest) * SCALE).astype(jnp.bfloat16)
        else:
            before = state[0][rows, :]
            largest = jnp.maximum(before, largest)
            shrink = jnp.exp2((before - largest) * SCALE)
            weights = jnp.exp2((scores - jnp.concatenate([largest] * (width(unit, n) // HD), 1)) * SCALE)
            weights = weights.astype(jnp.bfloat16)
        mixed = jnp.dot(weights, vw[: width(unit, n), :], preferred_element_type=jnp.float32)
        top, total = mixed[:, :HD], mixed[:, HD:]
        if not start:
            top = top + state[1][rows, :HD] * shrink
            total = total + state[1][rows, HD:] * shrink
        if last:
            store(unit, top, total)
        else:
            outs[0][rows, :] = jnp.broadcast_to(largest, (HEADS * QT, HD))
            outs[1][rows, :HD] = top
            outs[1][rows, HD:] = total

    def store(unit, top, total):
        tile, head = unit
        result = (top / total).astype(jnp.bfloat16)
        for i in range(HEADS):
            columns = slice((head + i) * HD, (head + i + 1) * HD)
            outs[0][tile * QT : tile * QT + QT, columns] = result[i * QT : (i + 1) * QT]

    units = [(tile, head) for tile in range(T // QT) for head in range(0, GROUP, HEADS)]

    def run(n):
        ahead = score(units[0], n)
        for i, unit in enumerate(units):
            scores, ahead = ahead, score(units[i + 1], n) if i + 1 < len(units) else None
            mix(unit, n, scores)

    def rest():
        if not last:
            outs[0][...] = state[0][...]
            outs[1][...] = state[1][...]
            return
        for tile, head in units:
            rows = slice((tile * GROUP + head) * QT, (tile * GROUP + head + HEADS) * QT)
            store((tile, head), state[1][rows, :HD], state[1][rows, HD:])

    if start:
        fetch.wait()
        run(1)
    else:
        for n in range(1, len(blocks) + 1):
            pl.when(count == n)(functools.partial(run, n))
        pl.when(count == 0)(rest)


STATE = [
    jax.ShapeDtypeStruct((GROUP * T, HD), jnp.float32),
    jax.ShapeDtypeStruct((GROUP * T, 2 * HD), jnp.float32),
]
RESULT = [jax.ShapeDtypeStruct((T, GROUP * HD), jnp.bfloat16)]


def in_hbm(x):
    return pltpu.with_memory_space_constraint(x, pltpu.HBM)


def stage(docs, queries, state, blocks, backs, causal=False, last=False):
    vmem = pl.BlockSpec(memory_space=pltpu.VMEM)
    start = not state
    out_shape = RESULT if last else STATE
    scratch = [pltpu.VMEM((len(blocks) * T, 2 * HD), jnp.bfloat16)] * 2
    if start:
        out_shape = [jax.ShapeDtypeStruct(queries.shape, queries.dtype)] + out_shape
        scratch.append(pltpu.SemaphoreType.DMA(()))
    args = (*state, *blocks)
    return pl.pallas_call(
        functools.partial(attend, causal, start, last, backs),
        out_shape=out_shape,
        in_specs=[vmem, pl.BlockSpec(memory_space=pltpu.HBM) if start else vmem]
        + [vmem] * len(args),
        out_specs=[vmem] * len(out_shape),
        scratch_shapes=scratch,
        compiler_params=pltpu.CompilerParams(vmem_limit_bytes=28 << 20),
        cost_estimate=pl.CostEstimate(
            flops=10**9 * len(blocks), transcendentals=10**6 * len(blocks), bytes_accessed=10**6
        ),
    )(docs, in_hbm(queries) if start else queries, *args)


def pack_kernel(k_ref, v_ref, lengths_ref, rows_ref, docs_ref, lengths, sems):
    copies = [
        pltpu.make_async_copy(lengths_ref, lengths, sems.at[0]),
        pltpu.make_async_copy(k_ref, rows_ref.at[:T, :], sems.at[1]),
        pltpu.make_async_copy(v_ref, rows_ref.at[T:, :], sems.at[2]),
    ]
    for copy in copies:
        copy.start()
    copies[0].wait()
    lane = lax.broadcasted_iota(jnp.int32, (1, LANES), 1)
    begins = jnp.full((1, LANES), 1 << 30, jnp.int32)
    ends = begins
    reached = jnp.int32(0)
    for i in range(lengths.shape[0]):
        begins = jnp.where(lane == i, reached, begins)
        reached = reached + lengths[i]
        ends = jnp.where(lane == i, reached, ends)
    docs_ref[0:1, :] = begins
    docs_ref[1:2, :] = ends
    copies[1].wait()
    copies[2].wait()


def pack(keys, values, doc_lengths):
    vmem = pl.BlockSpec(memory_space=pltpu.VMEM)
    return pl.pallas_call(
        pack_kernel,
        out_shape=[pltpu.VMEM((2 * T, HD), jnp.bfloat16), pltpu.VMEM((2, LANES), jnp.int32)],
        in_specs=[pl.BlockSpec(memory_space=pltpu.HBM)] * 3,
        out_specs=[vmem, vmem],
        scratch_shapes=[pltpu.SMEM(doc_lengths.shape, jnp.int32), pltpu.SemaphoreType.DMA((3,))],
        name="pack",
    )(*(in_hbm(x) for x in (keys, values, doc_lengths)))


def per_device(queries, key_rows, value_rows, doc_lengths):
    blocks = lax.axis_size("seq")
    rows, docs = pack(key_rows, value_rows, doc_lengths)
    a = lax.ppermute(rows, "seq", [(i, i + 2) for i in range(blocks - 2)])
    hops = [(i, i + 1 if i % 2 == 0 else i + 3) for i in range(blocks)]
    x = lax.ppermute(rows, "seq", [(i, j) for i, j in hops if j < blocks])
    s = lax.ppermute(a, "seq", [(i, i ^ 1) for i in range(blocks)])
    near, *state = stage(docs, queries, (), (rows,), ((0, 0),), causal=True)
    state = stage(docs, near, state, (a,), ((2, 2),))
    (merged,) = stage(docs, near, state, (s, x), ((1, 3), (3, 1)), last=True)
    return lax.all_to_all(merged, "head", split_axis=0, concat_axis=1, tiled=True)


def solution(mesh):
    in_specs = (P("seq", "head"), P("seq", "head"), P("seq", "head"), P())
    out_specs = P(("seq", "head"), None)
    return jax.shard_map(per_device, mesh=mesh, in_specs=in_specs, out_specs=out_specs, check_vma=False)
```

```python
import functools

import jax
import jax.numpy as jnp
from jax import lax
from jax.experimental import pallas as pl
from jax.experimental.pallas import tpu as pltpu
from jax.sharding import PartitionSpec as P


HD = 128
GROUP = 4
T = 512
LANES = 128
FAR = 4194304.0
SCALE = 0.08838834764831845 * 1.4426950408889634
QT = 256
HEADS = 4


def inside(docs_ref, base, rows):
    position = base + lax.broadcasted_iota(jnp.int32, (rows, LANES), 0)
    return (position >= docs_ref[0:1, :]) & (position < docs_ref[1:2, :])


def tabulate(lengths, docs_ref):
    lane = lax.broadcasted_iota(jnp.int32, (1, LANES), 1)
    begins = jnp.full((1, LANES), 1 << 30, jnp.int32)
    ends = begins
    reached = jnp.int32(0)
    for i in range(lengths.shape[0]):
        begins = jnp.where(lane == i, reached, begins)
        reached = reached + lengths[i]
        ends = jnp.where(lane == i, reached, ends)
    docs_ref[0:1, :] = begins
    docs_ref[1:2, :] = ends


def attend(causal, start, last, backs, docs_ref, q_ref, *refs):
    refs = list(refs)
    place = lax.axis_index("seq")
    first, odd = place * T, place % 2
    state = None if start else (refs.pop(0), refs.pop(0))
    blocks = [refs.pop(0) for _ in backs]
    if start:
        sems, lengths = refs.pop(), refs.pop()
        q_hbm, q_ref = q_ref, refs.pop(0)
        lengths_hbm, docs_ref = docs_ref, refs.pop(0)
        fetch = pltpu.make_async_copy(q_hbm, q_ref, sems.at[0])
        count_in = pltpu.make_async_copy(lengths_hbm, lengths, sems.at[1])
        count_in.start()
        fetch.start()
        count_in.wait()
        tabulate(lengths, docs_ref)
    kw, vw = refs[-2:]
    outs = refs[:-2]

    def put(slot, base, block):
        rows = pl.ds(pl.multiple_of(slot * T, T), T)
        kw[rows, :HD] = block[:T, :]
        kw[rows, HD:] = jnp.where(inside(docs_ref, base, T), 0.0, -FAR).astype(jnp.bfloat16)
        vw[rows, :HD] = block[T:, :]
        vw[rows, HD:] = jnp.ones((T, HD), jnp.bfloat16)

    count = 0
    if start:
        put(0, first, blocks[0])
    else:
        begins = docs_ref[0:1, :]
        reach = jnp.max(jnp.where(begins <= first, begins, 0).astype(jnp.float32))
        for block, (even_back, odd_back) in zip(blocks, backs):
            base = first - (even_back + odd * (odd_back - even_back)) * T
            needed = reach < (base + T).astype(jnp.float32)
            pl.when(needed)(functools.partial(put, count, base, block))
            count = count + needed.astype(jnp.int32)
    below = None
    if causal:
        row = lax.broadcasted_iota(jnp.int32, (HEADS * QT, QT), 0) % QT
        below = lax.broadcasted_iota(jnp.int32, (HEADS * QT, QT), 1) <= row
    owns = [
        jnp.where(inside(docs_ref, first + low, QT), 1.0, 0.0).astype(jnp.bfloat16) for low in range(0, T, QT)
    ]

    def width(unit, n):
        return unit[0] * QT + QT if causal else n * T

    def score(unit, n):
        tile, head = unit
        rows = slice(tile * QT, tile * QT + QT)
        query = jnp.concatenate(
            [
                jnp.concatenate([q_ref[rows, h * HD : (h + 1) * HD], owns[tile]], 1)
                for h in range(head, head + HEADS)
            ],
            0,
        )
        scores = lax.dot_general(
            query, kw[: width(unit, n), :], (((1,), (1,)), ((), ())), preferred_element_type=jnp.float32
        )
        if causal:
            low = tile * QT
            tail = jnp.where(below, scores[:, low:], -FAR)
            scores = tail if low == 0 else jnp.concatenate([scores[:, :low], tail], 1)
        return scores

    def mix(unit, n, scores):
        tile, head = unit
        at = (tile * GROUP + head) * QT
        rows = slice(at, at + HEADS * QT)
        largest = jnp.max(scores, axis=1, keepdims=True)
        if start:
            weights = jnp.exp2((scores - largest) * SCALE).astype(jnp.bfloat16)
        else:
            before = state[0][rows, :]
            largest = jnp.maximum(before, largest)
            shrink = jnp.exp2((before - largest) * SCALE)
            weights = jnp.exp2((scores - jnp.concatenate([largest] * (width(unit, n) // HD), 1)) * SCALE)
            weights = weights.astype(jnp.bfloat16)
        mixed = jnp.dot(weights, vw[: width(unit, n), :], preferred_element_type=jnp.float32)
        top, total = mixed[:, :HD], mixed[:, HD:]
        if not start:
            top = top + state[1][rows, :HD] * shrink
            total = total + state[1][rows, HD:] * shrink
        if last:
            store(unit, top, total)
        else:
            outs[0][rows, :] = jnp.broadcast_to(largest, (HEADS * QT, HD))
            outs[1][rows, :HD] = top
            outs[1][rows, HD:] = total

    def store(unit, top, total):
        tile, head = unit
        result = (top / total).astype(jnp.bfloat16)
        for i in range(HEADS):
            columns = slice((head + i) * HD, (head + i + 1) * HD)
            outs[0][tile * QT : tile * QT + QT, columns] = result[i * QT : (i + 1) * QT]

    units = [(tile, head) for tile in range(T // QT) for head in range(0, GROUP, HEADS)]

    def run(n):
        ahead = score(units[0], n)
        for i, unit in enumerate(units):
            scores, ahead = ahead, score(units[i + 1], n) if i + 1 < len(units) else None
            mix(unit, n, scores)

    def rest():
        if not last:
            outs[0][...] = state[0][...]
            outs[1][...] = state[1][...]
            return
        for tile, head in units:
            rows = slice((tile * GROUP + head) * QT, (tile * GROUP + head + HEADS) * QT)
            store((tile, head), state[1][rows, :HD], state[1][rows, HD:])

    if start:
        fetch.wait()
        run(1)
    else:
        for n in range(1, len(blocks) + 1):
            pl.when(count == n)(functools.partial(run, n))
        pl.when(count == 0)(rest)


STATE = [
    jax.ShapeDtypeStruct((GROUP * T, HD), jnp.float32),
    jax.ShapeDtypeStruct((GROUP * T, 2 * HD), jnp.float32),
]
RESULT = [jax.ShapeDtypeStruct((T, GROUP * HD), jnp.bfloat16)]


def in_hbm(x):
    return pltpu.with_memory_space_constraint(x, pltpu.HBM)


def stage(docs, queries, state, blocks, backs, causal=False, last=False):
    vmem = pl.BlockSpec(memory_space=pltpu.VMEM)
    start = not state
    out_shape = RESULT if last else STATE
    scratch = [pltpu.VMEM((len(blocks) * T, 2 * HD), jnp.bfloat16)] * 2
    if start:
        out_shape = [
            jax.ShapeDtypeStruct(queries.shape, queries.dtype),
            pltpu.VMEM((2, LANES), jnp.int32),
        ] + out_shape
        scratch += [pltpu.SMEM(docs.shape, jnp.int32), pltpu.SemaphoreType.DMA((2,))]
    args = (*state, *blocks)
    return pl.pallas_call(
        functools.partial(attend, causal, start, last, backs),
        out_shape=out_shape,
        in_specs=[pl.BlockSpec(memory_space=pltpu.HBM) if start else vmem] * 2 + [vmem] * len(args),
        out_specs=[vmem] * len(out_shape),
        scratch_shapes=scratch,
        compiler_params=pltpu.CompilerParams(vmem_limit_bytes=28 << 20),
        cost_estimate=pl.CostEstimate(
            flops=10**9 * len(blocks), transcendentals=10**6 * len(blocks), bytes_accessed=10**6
        ),
    )(*((in_hbm(docs), in_hbm(queries)) if start else (docs, queries)), *args)


def pack_kernel(k_ref, v_ref, rows_ref, sems):
    copies = [
        pltpu.make_async_copy(k_ref, rows_ref.at[:T, :], sems.at[0]),
        pltpu.make_async_copy(v_ref, rows_ref.at[T:, :], sems.at[1]),
    ]
    for copy in copies:
        copy.start()
    for copy in copies:
        copy.wait()


def pack(keys, values):
    vmem = pl.BlockSpec(memory_space=pltpu.VMEM)
    return pl.pallas_call(
        pack_kernel,
        out_shape=pltpu.VMEM((2 * T, HD), jnp.bfloat16),
        in_specs=[pl.BlockSpec(memory_space=pltpu.HBM)] * 2,
        out_specs=vmem,
        scratch_shapes=[pltpu.SemaphoreType.DMA((2,))],
        name="pack",
    )(in_hbm(keys), in_hbm(values))


def per_device(queries, key_rows, value_rows, doc_lengths):
    blocks = lax.axis_size("seq")
    rows = pack(key_rows, value_rows)
    a = lax.ppermute(rows, "seq", [(i, i + 2) for i in range(blocks - 2)])
    hops = [(i, i + 1 if i % 2 == 0 else i + 3) for i in range(blocks)]
    x = lax.ppermute(rows, "seq", [(i, j) for i, j in hops if j < blocks])
    s = lax.ppermute(a, "seq", [(i, i ^ 1) for i in range(blocks)])
    near, docs, *state = stage(doc_lengths, queries, (), (rows,), ((0, 0),), causal=True)
    state = stage(docs, near, state, (a,), ((2, 2),))
    (merged,) = stage(docs, near, state, (s, x), ((1, 3), (3, 1)), last=True)
    return lax.all_to_all(merged, "head", split_axis=0, concat_axis=1, tiled=True)


def solution(mesh):
    in_specs = (P("seq", "head"), P("seq", "head"), P("seq", "head"), P())
    out_specs = P(("seq", "head"), None)
    return jax.shard_map(per_device, mesh=mesh, in_specs=in_specs, out_specs=out_specs, check_vma=False)
```
